32 devices in a mesh: groups: 2 (over y), lon: 16 (over z, x, core).
Axes of the slice: x: 2, y: 2, z: 4, core: 2. Of those that a mesh axis runs over, the one named last changes fastest.
Arguments:
- fields: bfloat16 [4, 24, 192, 192], P('groups', None, 'lon'), parts along dimension 0, may hold values from -6 to 6
- norm_gain: float32 [192], replicated, may hold values from 0.25 to 1.75
- qkv_weight: bfloat16 [192, 576], replicated, may hold values from -2.5 to 2.5
- proj_weight: bfloat16 [192, 192], replicated, may hold values from -0.4375 to 0.4375
- bias_table: float32 [4, 6, 3312], replicated, may hold values from -4 to 4
- bias_index: int32 [144, 144], replicated, may hold values from 0 to 3311
- region_ids: int32 [2, 24], replicated, may hold values from 0 to 2
- mlp_gain: float32 [192], replicated, may hold values from 0.25 to 1.75
- up_weight: bfloat16 [192, 768], replicated, may hold values from -0.4375 to 0.4375
- down_weight: bfloat16 [768, 192], replicated, may hold values from -0.21875 to 0.21875
- merge_gain: float32 [768], replicated, may hold values from 0.25 to 1.75
- merge_weight: bfloat16 [768, 384], replicated, may hold values from -0.21875 to 0.21875
- cotangent: bfloat16 [4, 12, 96, 384], P('groups', None, 'lon'), parts along dimension 0, may hold values from -12 to 12
Outputs:
- merged: bfloat16 [4, 12, 96, 384], P('groups', None, 'lon'), parts along dimension 0
- field_grad: bfloat16 [4, 24, 192, 192], P('groups', None, 'lon'), parts along dimension 0
- qkv_grad: float32 [384, 576], P('groups'), parts along dimension 0
- proj_grad: float32 [384, 192], P('groups'), parts along dimension 0
- up_grad: float32 [384, 768], P('groups'), parts along dimension 0
- down_grad: float32 [1536, 192], P('groups'), parts along dimension 0
- merge_grad: float32 [1536, 384], P('groups'), parts along dimension 0
- table_grad: float32 [8, 6, 3312], P('groups'), parts along dimension 0
The draws below stay inside these ranges and needn't reach their ends.
There are 2 independent parts, one for each index of `groups`. The reference program is written for one: setup_inputs(seed, part) draws one part's arguments, and reference() takes and returns one part's arrays. A program takes and returns all parts, laid end to end along the dimension named above; an argument that names none is the same for every part. Nothing has to cross between parts.
All inputs are finite; a program needn't handle non-finite values.
Results may differ from the reference program's by a relative error of at most 0.019.
The reference program's roundings to bfloat16 on the way count: a program that leaves them out, or rounds other values in their place, can miss the bound.
Values may be sent and summed in bfloat16 or wider, within the bound.
A program may use at most 192 MiB of HBM per device.

```python
import jax
import jax.numpy as jnp
from jax import lax

C = 192
MLP = 768
HEADS = 6
HEAD = 32
WZ = 2
WLAT = 6
WLON = 12
HALF = 6
WIN = 144
BPOS = 3312
Z = 2
LAT = 24
NLON = 192
TYPES = 4


def draw_qkv_weight(key, part):
    entries = jnp.clip(jax.random.normal(key, (C, 3 * C), jnp.float32), -6.0, 6.0) * C ** (-0.5)
    entries = jnp.clip(entries, -2.5, 2.5)
    return entries.astype(jnp.bfloat16)


def draw_cotangent(key, part):
    dims_full = (Z, LAT // 2, NLON // 2, 2 * C)
    position = jnp.arange(NLON // 2).astype(jnp.float32) / (NLON // 2)
    rising = jnp.exp(jnp.log(3.0) * position)[None, None, :, None]
    noise_part = jnp.clip(jax.random.normal(key, dims_full, jnp.float32), -4.0, 4.0)
    return (noise_part * rising).astype(jnp.bfloat16)


def set_ends(array, stream_key, least, top_value):
    longest = array.shape.index(max(array.shape))
    spots = []
    for shift in (0, 1):
        where = [jax.random.randint(jax.random.fold_in(stream_key, axis), (), 0, length) for axis, length in enumerate(array.shape)]
        where[longest] = (where[longest] + shift) % array.shape[longest]
        spots.append(tuple(where))
    return array.at[spots[0]].set(least).at[spots[1]].set(top_value)


def steps_of(rng, shape, shards, least, top_value):
    gain = 1.0
    for dim, blocks in shards:
        draws = jax.random.uniform(jax.random.fold_in(jax.random.fold_in(rng, 6), dim), (blocks,), jnp.float32, least / len(shards), top_value / len(shards))
        gain = gain * jnp.repeat(jnp.exp(draws), shape[dim] // blocks).reshape((-1,) + (1,) * (len(shape) - 1 - dim))
    return gain


def bell_draw(rng, shape, scale, most, cuts=(), dtype=jnp.bfloat16):
    drawn = jax.random.normal(rng, shape, jnp.float32) * scale
    if len(cuts) > 0:
        drawn = steps_of(rng, shape, cuts, -0.22, 0.18) * drawn
    return jnp.clip(drawn, min=-most, max=most).astype(dtype)


def setup_inputs(seed: int = 0, part: int = 0) -> dict:
    streams_of = jax.random.split(jax.random.key(seed), 14)
    part_splits = jax.random.split(jax.random.fold_in(streams_of[13], part), 14)
    fields = bell_draw(part_splits[0], (Z, LAT, NLON, C), 1.0, 6.0, ((2, 16),))
    norm_gain = jnp.clip(1.0 + 0.15 * jax.random.normal(streams_of[1], (C,), jnp.float32), 0.25, 1.75)
    qkv_weight = draw_qkv_weight(jax.random.fold_in(streams_of[13], 71), part)
    proj_weight = bell_draw(streams_of[3], (C, C), C ** -0.5, 0.4375)
    bias_table = bell_draw(streams_of[4], (TYPES, HEADS, BPOS), 1.0, 4.0, (), jnp.float32)
    bias_index = set_ends(jax.random.randint(streams_of[5], (WIN, WIN), 0, BPOS), jax.random.fold_in(streams_of[5], 1), 0, BPOS - 1).astype(jnp.int32)
    region_ids = set_ends(jax.random.randint(streams_of[6], (Z, LAT), 0, 3), jax.random.fold_in(streams_of[6], 1), 0, 2).astype(jnp.int32)
    mlp_gain = jnp.clip(1.0 + 0.15 * jax.random.normal(streams_of[7], (C,), jnp.float32), 0.25, 1.75)
    up_weight = bell_draw(streams_of[8], (C, MLP), C ** -0.5, 0.4375)
    down_weight = bell_draw(streams_of[9], (MLP, C), MLP ** -0.5, 0.21875)
    merge_gain = jnp.clip(1.0 + 0.15 * jax.random.normal(streams_of[10], (4 * C,), jnp.float32), 0.25, 1.75)
    merge_weight = bell_draw(streams_of[11], (4 * C, 2 * C), (4 * C) ** -0.5, 0.21875)
    cotangent = draw_cotangent(jax.random.fold_in(jax.random.fold_in(streams_of[13], part), 71), part)
    return {"fields": fields, "norm_gain": norm_gain, "qkv_weight": qkv_weight, "proj_weight": proj_weight, "bias_table": bias_table, "bias_index": bias_index, "region_ids": region_ids, "mlp_gain": mlp_gain, "up_weight": up_weight, "down_weight": down_weight, "merge_gain": merge_gain, "merge_weight": merge_weight, "cotangent": cotangent}


def layer_norm(values, norm_gain):
    average = lax.optimization_barrier(jnp.mean(values, axis=-1, keepdims=True))
    centred = values - average
    variance = lax.optimization_barrier(jnp.mean(centred * centred, axis=-1, keepdims=True))
    return centred * lax.rsqrt(variance + 1e-05) * norm_gain

def to_windows(grid_in):
    levels, latitudes, longitudes, features = grid_in.shape
    blocks = grid_in.reshape(levels // WZ, WZ, latitudes // WLAT, WLAT, longitudes // WLON, WLON, features)
    blocks = blocks.transpose(0, 2, 4, 1, 3, 5, 6)
    return blocks.reshape(levels // WZ * (latitudes // WLAT), longitudes // WLON, WIN, features)

def from_windows(windows, levels, latitudes):
    number = windows.shape[1]
    features = windows.shape[3]
    blocks = windows.reshape(levels // WZ, latitudes // WLAT, number, WZ, WLAT, WLON, features)
    blocks = blocks.transpose(0, 3, 1, 4, 2, 5, 6)
    return blocks.reshape(levels, latitudes, number * WLON, features)

def region_mask(region_ids):
    labels = region_ids.reshape(Z // WZ, WZ, LAT // WLAT, WLAT).transpose(0, 2, 1, 3)
    labels = jnp.repeat(labels.reshape(TYPES, WZ * WLAT), WLON, axis=1)
    return labels[:, :, None] == labels[:, None, :]

def regroup(grid_in):
    levels, latitudes, longitudes, features = grid_in.shape
    blocks = grid_in.reshape(levels, latitudes // 2, 2, longitudes // 2, 2, features)
    return blocks.transpose(0, 1, 3, 2, 4, 5).reshape(levels, latitudes // 2, longitudes // 2, 4 * features)

def attend_one(tokens_win, qkv_weight, proj_weight, bias_rows, same_region, probe_qkv, probe_proj):
    triple = (jnp.dot(tokens_win, qkv_weight, preferred_element_type=jnp.float32) + probe_qkv).astype(jnp.bfloat16)
    shaped = triple.reshape(tokens_win.shape[:2] + (3, HEADS, HEAD)).astype(jnp.float32)
    scores = jnp.einsum('wqhd,wkhd->whqk', shaped[:, :, 0], shaped[:, :, 1]) * HEAD ** (-0.5) + bias_rows
    scores = jnp.where(same_region, scores, -1e+30)
    row_max = lax.optimization_barrier(jnp.max(scores, axis=-1, keepdims=True))
    weights = jnp.exp(scores - row_max)
    probability = (weights / lax.optimization_barrier(jnp.sum(weights, axis=-1, keepdims=True))).astype(jnp.bfloat16)
    mixed_heads = jnp.einsum('whqk,wkhd->wqhd', probability.astype(jnp.float32), shaped[:, :, 2])
    mixed_heads = mixed_heads.astype(jnp.bfloat16).reshape(tokens_win.shape)
    result = jnp.dot(mixed_heads, proj_weight, preferred_element_type=jnp.float32) + probe_proj
    return (result.astype(jnp.bfloat16), mixed_heads)

def weight_term(inputs, grads):
    rows_in = inputs.reshape(-1, inputs.shape[-1])
    rows_out = grads.reshape(-1, grads.shape[-1]).astype(jnp.bfloat16)
    return jnp.dot(rows_in.T, rows_out, preferred_element_type=jnp.float32)

def table_sums(grad_bias, bias_index):
    flat = grad_bias.reshape(TYPES * HEADS, WIN * WIN).T
    summed = jax.ops.segment_sum(flat, bias_index.reshape(-1), num_segments=BPOS)
    return summed.T.reshape(TYPES, HEADS, BPOS)

def reference(fields, norm_gain, qkv_weight, proj_weight, bias_table, bias_index, region_ids, mlp_gain, up_weight, down_weight, merge_gain, merge_weight, cotangent):
    same_region = region_mask(region_ids)
    bias_rows = jnp.take(bias_table, bias_index, axis=2)

    def forward(fields_in, bias_in, probes):
        probe_qkv, probe_proj, probe_up, probe_down, probe_merge = probes
        field_f32 = fields_in.astype(jnp.float32)
        normed = layer_norm(field_f32, norm_gain).astype(jnp.bfloat16)
        rolled = jnp.roll(normed, -HALF, axis=2)
        tokens_win = to_windows(rolled)

        def per_type(parts):
            return attend_one(parts[0], qkv_weight, proj_weight, parts[1][None], parts[2], parts[3], parts[4])
        result, mixed_heads = lax.map(jax.checkpoint(per_type), (tokens_win, bias_in, same_region, probe_qkv, probe_proj))
        branch = jnp.roll(from_windows(result, Z, LAT), HALF, axis=2)
        after_attn = lax.optimization_barrier((field_f32 + branch.astype(jnp.float32)).astype(jnp.bfloat16))
        after_f32 = after_attn.astype(jnp.float32)
        normed_mlp = layer_norm(after_f32, mlp_gain).astype(jnp.bfloat16)
        hidden = jax.nn.gelu(jnp.dot(normed_mlp, up_weight, preferred_element_type=jnp.float32) + probe_up, approximate=False).astype(jnp.bfloat16)
        after_mlp = (after_f32 + jnp.dot(hidden, down_weight, preferred_element_type=jnp.float32) + probe_down).astype(jnp.bfloat16)
        normed_merge = layer_norm(regroup(after_mlp).astype(jnp.float32), merge_gain).astype(jnp.bfloat16)
        merged = (jnp.dot(normed_merge, merge_weight, preferred_element_type=jnp.float32) + probe_merge).astype(jnp.bfloat16)
        return (merged, (tokens_win, mixed_heads, normed_mlp, hidden, normed_merge))
    windows_lon = NLON // WLON
    probes = (jnp.zeros((TYPES, windows_lon, WIN, 3 * C), jnp.float32), jnp.zeros((TYPES, windows_lon, WIN, C), jnp.float32), jnp.zeros((Z, LAT, NLON, MLP), jnp.float32), jnp.zeros((Z, LAT, NLON, C), jnp.float32), jnp.zeros((Z, LAT // 2, NLON // 2, 2 * C), jnp.float32))
    merged, backward, stored = jax.vjp(forward, fields, bias_rows, probes, has_aux=True)
    field_grad, grad_bias, grad_probes = backward(cotangent)
    tokens_win, mixed_heads, normed_mlp, hidden, normed_merge = stored
    grad_qkv, grad_proj, grad_up, grad_down, grad_merge = grad_probes
    factor = float(Z * LAT * NLON) ** (-0.5)
    qkv_grad = weight_term(tokens_win, grad_qkv) * factor
    proj_grad = weight_term(mixed_heads, grad_proj) * factor
    up_grad = weight_term(normed_mlp, grad_up) * factor
    down_grad = weight_term(hidden, grad_down) * factor
    merge_grad = weight_term(normed_merge, grad_merge) * factor
    table_grad = table_sums(grad_bias, bias_index) * factor
    return (merged, field_grad, qkv_grad, proj_grad, up_grad, down_grad, merge_grad, table_grad)
```

```python
import functools

import jax
import jax.numpy as jnp
import numpy as np
from jax import lax
from jax.experimental import pallas as pl
from jax.experimental.pallas import tpu as pltpu
from jax.sharding import PartitionSpec as P

C = 192
MLP = 768
HEADS = 6
HEAD = 32
WZ = 2
WLAT = 6
WLON = 12
HALF = 6
WIN = 144
BPOS = 3312
Z = 2
LAT = 24
TYPES = 4
TH = TYPES * HEADS
LANES = 128
KEYS = 256
RADIX = 256
DIGITS = -(-BPOS // RADIX)
GROUP = WIN // 4
GPAD = 48
ROWS_W = 30 * C
ROWS_T = DIGITS * TH * 2
BF = jnp.bfloat16
F32 = jnp.float32
VMEM = pl.BlockSpec(memory_space=pltpu.VMEM)


def dot(a, b, dims=((1,), (0,))):
    return lax.dot_general(a, b, (dims, ((), ())), preferred_element_type=F32)


NT = ((1,), (1,))
TN = ((0,), (0,))


def bias_kernel(high_ref, low_ref, digit_ref, lane_ref, out_ref):
    def row(i, carry):
        lane = lane_ref[pl.ds(i, 1), :]
        digit = digit_ref[pl.ds(i, 1), :]
        hot = (lax.broadcasted_iota(jnp.int32, (RADIX, KEYS), 0) == lane).astype(BF)
        high = dot(high_ref[...], hot)
        low = dot(low_ref[...], hot)
        total = jnp.zeros((TH, KEYS), F32)
        for d in range(DIGITS):
            piece = high[d * TH:(d + 1) * TH] + low[d * TH:(d + 1) * TH]
            total = jnp.where(digit == d, piece, total)
        rows = pl.ds(pl.multiple_of(i * TH, TH), TH)
        out_ref[0, rows, :] = total[:, :LANES]
        out_ref[1, rows, :] = total[:, LANES:]
        return carry

    lax.fori_loop(0, WIN, row, 0)


def norm_parts(values):
    average = jnp.mean(values, axis=-1, keepdims=True)
    centred = values - average
    variance = jnp.mean(centred * centred, axis=-1, keepdims=True)
    scale = lax.rsqrt(variance + 1e-05)
    return centred * scale, scale


def norm_grad(hat, scale, grad_hat):
    first = jnp.mean(grad_hat, axis=-1, keepdims=True)
    second = jnp.mean(grad_hat * hat, axis=-1, keepdims=True)
    return scale * (grad_hat - first - hat * second)


def block_kernel(
    x_ref, ct_ref, bias_ref, regq_ref, regk_ref, digit_ref, lane_ref, perm_ref,
    g1_ref, wqkv_ref, wproj_ref, g2_ref, wup_ref, wdown_ref, gm_ref, wm_ref,
    merged_ref, fgrad_ref, packed_ref,
    triple, prob, mixed, dmixed, dtriple, dscore,
    s_normed, s_dtriple, s_mixed, s_da, s_nmlp, s_du, s_hidden, s_dy, s_merge, s_table,
):
    s_merge[...] = jnp.zeros_like(s_merge)
    triple[...] = jnp.zeros_like(triple)
    root = float(HEAD) ** (-0.5)

    def one_type(t, carry):
        rows = pl.ds(pl.multiple_of(t * WIN, 16), WIN)
        field = x_ref[rows, :].astype(F32)
        hat1, scale1 = norm_parts(field)
        normed = (hat1 * g1_ref[...]).astype(BF)
        s_normed[rows, :] = normed
        triple[0:WIN, :] = dot(normed, wqkv_ref[...]).astype(BF)
        same = regq_ref[t] == regk_ref[t]
        for h in range(HEADS):
            q = triple[0:WIN, h * HEAD:(h + 1) * HEAD]
            k = triple[:, C + h * HEAD:C + (h + 1) * HEAD]
            v = triple[:, 2 * C + h * HEAD:2 * C + (h + 1) * HEAD]
            where_rows = pl.ds(t * HEADS + h, WIN, stride=TH)
            bias = jnp.concatenate(
                [bias_ref[0, where_rows, :], bias_ref[1, where_rows, :]], axis=1
            )
            scores = jnp.where(same, dot(q, k, NT) * root + bias, -1e30)
            weights = jnp.exp(scores - jnp.max(scores, axis=-1, keepdims=True))
            p = weights / jnp.sum(weights, axis=-1, keepdims=True)
            prob[h] = p
            mixed[:, h * HEAD:(h + 1) * HEAD] = dot(p.astype(BF), v).astype(BF)
        mixed_heads = mixed[...]
        s_mixed[rows, :] = mixed_heads
        branch = dot(mixed_heads, wproj_ref[...]).astype(BF).astype(F32)
        after = (field + branch).astype(BF).astype(F32)
        hat2, scale2 = norm_parts(after)
        nmlp = (hat2 * g2_ref[...]).astype(BF)
        s_nmlp[rows, :] = nmlp
        up = dot(nmlp, wup_ref[...])
        cdf = 0.5 * (1.0 + lax.erf(up * np.float32(np.sqrt(0.5))))
        slope = cdf + up * (jnp.exp(-0.5 * up * up) * np.float32(1 / np.sqrt(2 * np.pi)))
        hidden = (up * cdf).astype(BF)
        s_hidden[rows, :] = hidden
        after_mlp = (after + dot(hidden, wdown_ref[...])).astype(BF)

        spread = dot(perm_ref[...], after_mlp)
        parts = [spread[g * GPAD:(g + 1) * GPAD] for g in range(4)]
        average = sum(jnp.sum(p, axis=-1, keepdims=True) for p in parts) / (4 * C)
        parts = [p - average for p in parts]
        variance = sum(jnp.sum(p * p, axis=-1, keepdims=True) for p in parts) / (4 * C)
        scale = lax.rsqrt(variance + 1e-05)
        hats = [p * scale for p in parts]
        ct = ct_ref[t]
        merged = jnp.zeros((GPAD, 2 * C), F32)
        grads = []
        for g in range(4):
            gain = gm_ref[g:g + 1, :]
            weight = wm_ref[g * C:(g + 1) * C, :]
            nm = (hats[g] * gain).astype(BF)
            merged = merged + dot(nm, weight)
            s_merge[g * C:(g + 1) * C, :] += dot(nm, ct, TN)
            grads.append(dot(ct, weight, NT).astype(BF).astype(F32) * gain)
        merged_ref[t] = merged.astype(BF)
        first = sum(jnp.sum(g, axis=-1, keepdims=True) for g in grads) / (4 * C)
        second = sum(
            jnp.sum(g * hat, axis=-1, keepdims=True) for g, hat in zip(grads, hats)
        ) / (4 * C)
        back = jnp.concatenate(
            [scale * (g - first - hat * second) for g, hat in zip(grads, hats)], axis=0
        ).astype(BF)
        dy = dot(perm_ref[...], back, TN).astype(BF)

        s_dy[rows, :] = dy
        dhidden = dot(dy, wdown_ref[...], NT).astype(BF).astype(F32)
        du = (dhidden * slope).astype(BF)
        s_du[rows, :] = du
        dn = dot(du, wup_ref[...], NT).astype(BF).astype(F32) * g2_ref[...]
        da = (dy.astype(F32) + norm_grad(hat2, scale2, dn)).astype(BF)
        s_da[rows, :] = da

        dmixed[...] = dot(da, wproj_ref[...], NT).astype(BF)
        for h in range(HEADS):
            q = triple[0:WIN, h * HEAD:(h + 1) * HEAD]
            k = triple[:, C + h * HEAD:C + (h + 1) * HEAD]
            v = triple[:, 2 * C + h * HEAD:2 * C + (h + 1) * HEAD]
            dm = dmixed[:, h * HEAD:(h + 1) * HEAD]
            p = prob[h]
            dp = dot(dm, v, NT).astype(BF).astype(F32)
            ds = p * (dp - jnp.sum(dp * p, axis=-1, keepdims=True))
            where_rows = pl.ds(t * HEADS + h, WIN, stride=TH)
            dscore[0, where_rows, :] = ds[:, :LANES]
            dscore[1, where_rows, :] = ds[:, LANES:]
            dsb = (ds * root).astype(BF)
            dtriple[:, h * HEAD:(h + 1) * HEAD] = dot(dsb, k).astype(BF)
            dtriple[:, C + h * HEAD:C + (h + 1) * HEAD] = dot(dsb, q, TN)[:WIN].astype(BF)
            dtriple[:, 2 * C + h * HEAD:2 * C + (h + 1) * HEAD] = dot(
                p.astype(BF), dm, TN
            )[:WIN].astype(BF)
        dt = dtriple[...]
        s_dtriple[rows, :] = dt
        dn1 = dot(dt, wqkv_ref[...], NT).astype(BF).astype(F32) * g1_ref[...]
        fgrad_ref[rows, :] = (da.astype(F32) + norm_grad(hat1, scale1, dn1)).astype(BF)
        return carry

    lax.fori_loop(0, TYPES, one_type, 0)

    def pack(first_block, value):
        for b in range(value.shape[1] // LANES):
            start = (first_block + b) * C
            packed_ref[start:start + C, :] = value[:, b * LANES:(b + 1) * LANES].astype(BF)

    pack(0, jnp.concatenate(
        [dot(s_normed[...], s_dtriple[...], TN), dot(s_mixed[...], s_da[...], TN)], axis=1))
    pack(6, dot(s_nmlp[...], s_du[...], TN))
    down = dot(s_hidden[...], s_dy[...], TN)
    pack(12, jnp.concatenate([down[g * C:(g + 1) * C] for g in range(4)], axis=1))
    for g in range(4):
        pack(18 + 3 * g, s_merge[g * C:(g + 1) * C, :])

    s_table[...] = jnp.zeros_like(s_table)

    def row(i, carry):
        lane = lane_ref[pl.ds(i, 1), :]
        digit = digit_ref[pl.ds(i, 1), :]
        hot = (lax.broadcasted_iota(jnp.int32, (RADIX, KEYS), 0) == lane).astype(BF)
        rows = pl.ds(pl.multiple_of(i * TH, TH), TH)
        ds = jnp.concatenate([dscore[0, rows, :], dscore[1, rows, :]], axis=1)
        left = jnp.concatenate(
            [jnp.where(digit == d, ds, 0.0) for d in range(DIGITS)], axis=0
        ).astype(BF)
        s_table[...] += dot(left, hot, NT)
        return carry

    lax.fori_loop(0, WIN, row, 0)
    for b in range(2):
        start = ROWS_W + b * DIGITS * TH
        packed_ref[start:start + DIGITS * TH, :] = s_table[:, b * LANES:(b + 1) * LANES].astype(BF)
    end = ROWS_W + ROWS_T
    if packed_ref.shape[0] > end:
        packed_ref[end:, :] = jnp.zeros((packed_ref.shape[0] - end, LANES), BF)


def reduce_kernel(
    n, share, factor, packed_ref,
    qkv_ref, proj_ref, up_ref, down_ref, merge_ref, table_ref,
    arrived, gathered, send1, recv1, send2, recv2,
):
    me = lax.axis_index("lon")
    barrier = pltpu.get_barrier_semaphore()
    for k in range(1, n):
        pl.semaphore_signal(
            barrier, inc=1, device_id={"lon": lax.rem(me + k, n)},
            device_id_type=pl.DeviceIdType.MESH,
        )
    pl.semaphore_wait(barrier, n - 1)

    def rows_of(device):
        return pl.ds(pl.multiple_of(device * share, 16), share)

    first = []
    for k in range(1, n):
        peer = lax.rem(me + k, n)
        copy = pltpu.make_async_remote_copy(
            src_ref=packed_ref.at[rows_of(peer), :], dst_ref=arrived.at[k],
            send_sem=send1.at[k], recv_sem=recv1.at[k],
            device_id={"lon": peer}, device_id_type=pl.DeviceIdType.MESH,
        )
        copy.start()
        first.append(copy)
    for copy in first:
        copy.wait_recv()
    total = packed_ref[rows_of(me), :].astype(F32)
    for k in range(1, n):
        total = total + arrived[k].astype(F32)
    gathered[rows_of(me), :] = total.astype(BF)
    second = []
    for k in range(1, n):
        copy = pltpu.make_async_remote_copy(
            src_ref=gathered.at[rows_of(me), :], dst_ref=gathered.at[rows_of(me), :],
            send_sem=send2.at[k], recv_sem=recv2.at[k],
            device_id={"lon": lax.rem(me + k, n)}, device_id_type=pl.DeviceIdType.MESH,
        )
        copy.start()
        second.append(copy)
    for copy in first:
        copy.wait_send()
    for copy in second:
        copy.wait()

    def block(index):
        return gathered[index * C:(index + 1) * C, :].astype(F32) * factor

    def joined(start, count):
        return jnp.concatenate([block(start + b) for b in range(count)], axis=1)

    front = joined(0, 6)
    qkv_ref[...] = front[:, :3 * C]
    proj_ref[...] = front[:, 3 * C:]
    up_ref[...] = joined(6, 6)
    downs = joined(12, 6)
    for g in range(4):
        down_ref[g * C:(g + 1) * C, :] = downs[:, g * C:(g + 1) * C]
        merge_ref[g * C:(g + 1) * C, :] = joined(18 + 3 * g, 3)
    for b in range(2):
        start = ROWS_W + b * DIGITS * TH
        half = gathered[start:start + DIGITS * TH, :].astype(F32) * factor
        for d in range(DIGITS):
            at = d * RADIX + b * LANES
            table_ref[:, at:at + LANES] = half[d * TH:(d + 1) * TH]


def passed_along(value, axis, steps):
    count = lax.axis_size(axis)
    return lax.ppermute(value, axis, [(s, (s + steps) % count) for s in range(count)])


def group_order():
    order = np.zeros((4 * GPAD, WIN), np.float32)
    for pa in range(2):
        for pb in range(2):
            for z in range(WZ):
                for a in range(WLAT // 2):
                    for b in range(WLON // 2):
                        cell = (z * (WLAT // 2) + a) * (WLON // 2) + b
                        token = (z * WLAT + 2 * a + pa) * WLON + 2 * b + pb
                        order[(2 * pa + pb) * GPAD + cell, token] = 1.0
    return jnp.asarray(order, BF)


def local(
    fields, norm_gain, qkv_weight, proj_weight, bias_table, bias_index, region_ids,
    mlp_gain, up_weight, down_weight, merge_gain, merge_weight, cotangent,
):
    n = lax.axis_size("lon")
    windows = fields.shape[2] // WLON
    assert windows == 1
    bands = LAT // WLAT
    west_fields = passed_along(fields[:, :, :HALF], "lon", -1)
    west_ct = passed_along(cotangent[:, :, :HALF // 2], "lon", -1)

    table = jnp.pad(bias_table.reshape(TH, BPOS), ((0, 0), (0, DIGITS * RADIX - BPOS)))
    table = table.reshape(TH, DIGITS, RADIX).transpose(1, 0, 2).reshape(DIGITS * TH, RADIX)
    high = lax.reduce_precision(table, 8, 7)
    low = (table - high).astype(BF)
    high = high.astype(BF)
    index = jnp.pad(bias_index, ((0, 0), (0, KEYS - WIN)), constant_values=-1)
    digit = index >> 8
    lane = jnp.where(index < 0, -1, index & (RADIX - 1))
    bias = pl.pallas_call(
        bias_kernel,
        out_shape=jax.ShapeDtypeStruct((2, WIN * TH, LANES), F32),
        in_specs=[VMEM] * 4,
        out_specs=VMEM,
        compiler_params=pltpu.CompilerParams(vmem_limit_bytes=24 << 20),
        cost_estimate=pl.CostEstimate(flops=14_000_000_000, bytes_accessed=4 << 20, transcendentals=0),
        name="bias_rows",
    )(high, low, digit, lane)

    labels = region_ids.reshape(WZ, bands, WLAT).transpose(1, 0, 2).reshape(TYPES, WZ * WLAT)
    labels = jnp.repeat(labels, WLON, axis=1)
    label_keys = jnp.pad(labels, ((0, 0), (0, KEYS - WIN)), constant_values=-1)

    shifted = jnp.concatenate([fields[:, :, HALF:], west_fields], axis=2)
    tokens = shifted.reshape(WZ, bands, WLAT, WLON, C).transpose(1, 0, 2, 3, 4).reshape(TYPES * WIN, C)
    ct = jnp.concatenate([cotangent[:, :, HALF // 2:], west_ct], axis=2)
    ct = ct.reshape(WZ, bands, WLAT // 2, WLON // 2, 2 * C).transpose(1, 0, 2, 3, 4)
    ct = jnp.pad(ct.reshape(TYPES, GROUP, 2 * C), ((0, 0), (0, GPAD - GROUP), (0, 0)))

    share = -(-(ROWS_W + ROWS_T) // (16 * n)) * 16
    total_rows = TYPES * WIN
    merged_win, fgrad_win, packed = pl.pallas_call(
        block_kernel,
        out_shape=(
            jax.ShapeDtypeStruct((TYPES, GPAD, 2 * C), BF),
            jax.ShapeDtypeStruct((total_rows, C), BF),
            jax.ShapeDtypeStruct((n * share, LANES), BF),
        ),
        in_specs=[VMEM] * 16,
        out_specs=(VMEM,) * 3,
        scratch_shapes=[
            pltpu.VMEM((KEYS, 3 * C), BF),
            pltpu.VMEM((HEADS, WIN, KEYS), F32),
            pltpu.VMEM((WIN, C), BF),
            pltpu.VMEM((WIN, C), BF),
            pltpu.VMEM((WIN, 3 * C), BF),
            pltpu.VMEM((2, WIN * TH, LANES), F32),
            pltpu.VMEM((total_rows, C), BF),
            pltpu.VMEM((total_rows, 3 * C), BF),
            pltpu.VMEM((total_rows, C), BF),
            pltpu.VMEM((total_rows, C), BF),
            pltpu.VMEM((total_rows, C), BF),
            pltpu.VMEM((total_rows, MLP), BF),
            pltpu.VMEM((total_rows, MLP), BF),
            pltpu.VMEM((total_rows, C), BF),
            pltpu.VMEM((4 * C, 2 * C), F32),
            pltpu.VMEM((DIGITS * TH, RADIX), F32),
        ],
        compiler_params=pltpu.CompilerParams(vmem_limit_bytes=48 << 20),
        cost_estimate=pl.CostEstimate(flops=20_000_000_000, bytes_accessed=8 << 20, transcendentals=2_000_000),
        name="block",
    )(
        tokens, ct, bias, labels[:, :, None], label_keys[:, None, :], digit, lane, group_order(),
        norm_gain[None], qkv_weight, proj_weight, mlp_gain[None], up_weight, down_weight,
        merge_gain.reshape(4, C), merge_weight,
    )

    merged_grid = merged_win[:, :GROUP].reshape(bands, WZ, WLAT // 2, WLON // 2, 2 * C)
    merged_grid = merged_grid.transpose(1, 0, 2, 3, 4).reshape(Z, LAT // 2, WLON // 2, 2 * C)
    fgrad_grid = fgrad_win.reshape(bands, WZ, WLAT, WLON, C)
    fgrad_grid = fgrad_grid.transpose(1, 0, 2, 3, 4).reshape(Z, LAT, WLON, C)
    east_merged = passed_along(merged_grid[:, :, HALF // 2:], "lon", 1)
    east_fgrad = passed_along(fgrad_grid[:, :, HALF:], "lon", 1)
    merged = jnp.concatenate([east_merged, merged_grid[:, :, :HALF // 2]], axis=2)
    field_grad = jnp.concatenate([east_fgrad, fgrad_grid[:, :, :HALF]], axis=2)

    factor = float(Z * LAT * fields.shape[2] * n) ** (-0.5)
    outs = pl.pallas_call(
        functools.partial(reduce_kernel, n, share, factor),
        out_shape=(
            jax.ShapeDtypeStruct((C, 3 * C), F32),
            jax.ShapeDtypeStruct((C, C), F32),
            jax.ShapeDtypeStruct((C, MLP), F32),
            jax.ShapeDtypeStruct((MLP, C), F32),
            jax.ShapeDtypeStruct((4 * C, 2 * C), F32),
            jax.ShapeDtypeStruct((TH, DIGITS * RADIX), F32),
        ),
        in_specs=[VMEM],
        out_specs=(VMEM,) * 6,
        scratch_shapes=[
            pltpu.VMEM((n, share, LANES), BF),
            pltpu.VMEM((n * share, LANES), BF),
            pltpu.SemaphoreType.DMA((n,)),
            pltpu.SemaphoreType.DMA((n,)),
            pltpu.SemaphoreType.DMA((n,)),
            pltpu.SemaphoreType.DMA((n,)),
        ],
        compiler_params=pltpu.CompilerParams(
            collective_id=0, has_side_effects=True, vmem_limit_bytes=24 << 20
        ),
        cost_estimate=pl.CostEstimate(flops=10_000_000_000, bytes_accessed=16 << 20, transcendentals=0),
        name="weight_sums",
    )(packed)
    qkv_grad, proj_grad, up_grad, down_grad, merge_grad, table_grad = outs
    table_grad = table_grad[:, :BPOS].reshape(TYPES, HEADS, BPOS)
    return (
        merged, field_grad, qkv_grad, proj_grad, up_grad, down_grad, merge_grad, table_grad,
    )


def solution(mesh):
    grid = P("groups", None, "lon", None)
    rows = P("groups", None)
    return jax.shard_map(
        local,
        mesh=mesh,
        in_specs=(grid,) + (P(),) * 11 + (grid,),
        out_specs=(grid, grid) + (rows,) * 5 + (P("groups", None, None),),
        check_vma=False,
    )
```

```python
import functools

import jax
import jax.numpy as jnp
import numpy as np
from jax import lax
from jax.experimental import pallas as pl
from jax.experimental.pallas import tpu as pltpu
from jax.sharding import PartitionSpec as P

C = 192
MLP = 768
HEADS = 6
HEAD = 32
WZ = 2
WLAT = 6
WLON = 12
HALF = 6
WIN = 144
BPOS = 3312
Z = 2
LAT = 24
TYPES = 4
TH = TYPES * HEADS
LANES = 128
KEYS = 256
RADIX = 256
DIGITS = -(-BPOS // RADIX)
GROUP = WIN // 4
GPAD = 48
ROWS_W = 30 * C
ROWS_T = DIGITS * TH * 2
UNROLL = 4
BF = jnp.bfloat16
F32 = jnp.float32
VMEM = pl.BlockSpec(memory_space=pltpu.VMEM)


def dot(a, b, dims=((1,), (0,))):
    return lax.dot_general(a, b, (dims, ((), ())), preferred_element_type=F32)


NT = ((1,), (1,))
TN = ((0,), (0,))


def bias_kernel(table_ref, digit_ref, lane_ref, out_ref):
    def some_rows(step, carry):
        for u in range(UNROLL):
            i = step * UNROLL + u
            lane = lane_ref[pl.ds(i, 1), :]
            digit = digit_ref[pl.ds(i, 1), :]
            hot = (lax.broadcasted_iota(jnp.int32, (RADIX, KEYS), 0) == lane).astype(BF)
            found = dot(table_ref[...], hot)
            total = jnp.zeros((TH, KEYS), F32)
            for d in range(DIGITS):
                total = jnp.where(digit == d, found[d * TH:(d + 1) * TH], total)
            rows = pl.ds(pl.multiple_of(i * TH, TH), TH)
            out_ref[0, rows, :] = total[:, :LANES]
            out_ref[1, rows, :] = total[:, LANES:]
        return carry

    lax.fori_loop(0, WIN // UNROLL, some_rows, 0)


def norm_parts(values):
    average = jnp.mean(values, axis=-1, keepdims=True)
    centred = values - average
    variance = jnp.mean(centred * centred, axis=-1, keepdims=True)
    scale = lax.rsqrt(variance + 1e-05)
    return centred * scale, scale


def norm_grad(hat, scale, grad_hat):
    first = jnp.mean(grad_hat, axis=-1, keepdims=True)
    second = jnp.mean(grad_hat * hat, axis=-1, keepdims=True)
    return scale * (grad_hat - first - hat * second)


def block_kernel(
    x_ref, ct_ref, bias_ref, regq_ref, regk_ref, digit_ref, lane_ref, perm_ref,
    g1_ref, wqkv_ref, wproj_ref, g2_ref, wup_ref, wdown_ref, gm_ref, wm_ref,
    merged_ref, fgrad_ref, packed_ref,
    triple, prob, mixed, dmixed, dtriple, dscore,
    s_normed, s_dtriple, s_mixed, s_da, s_nmlp, s_du, s_hidden, s_dy, s_merge, s_table,
):
    s_merge[...] = jnp.zeros_like(s_merge)
    triple[...] = jnp.zeros_like(triple)
    root = float(HEAD) ** (-0.5)

    def one_type(t, carry):
        rows = pl.ds(pl.multiple_of(t * WIN, 16), WIN)
        field = x_ref[rows, :].astype(F32)
        hat1, scale1 = norm_parts(field)
        normed = (hat1 * g1_ref[...]).astype(BF)
        s_normed[rows, :] = normed
        triple[0:WIN, :] = dot(normed, wqkv_ref[...]).astype(BF)
        same = regq_ref[t] == regk_ref[t]
        for h in range(HEADS):
            q = triple[0:WIN, h * HEAD:(h + 1) * HEAD]
            k = triple[:, C + h * HEAD:C + (h + 1) * HEAD]
            v = triple[:, 2 * C + h * HEAD:2 * C + (h + 1) * HEAD]
            where_rows = pl.ds(t * HEADS + h, WIN, stride=TH)
            bias = jnp.concatenate(
                [bias_ref[0, where_rows, :], bias_ref[1, where_rows, :]], axis=1
            )
            scores = jnp.where(same, dot(q, k, NT) * root + bias, -1e30)
            weights = jnp.exp(scores - jnp.max(scores, axis=-1, keepdims=True))
            p = weights / jnp.sum(weights, axis=-1, keepdims=True)
            prob[h] = p
            mixed[:, h * HEAD:(h + 1) * HEAD] = dot(p.astype(BF), v).astype(BF)
        mixed_heads = mixed[...]
        s_mixed[rows, :] = mixed_heads
        branch = dot(mixed_heads, wproj_ref[...]).astype(BF).astype(F32)
        after = (field + branch).astype(BF).astype(F32)
        hat2, scale2 = norm_parts(after)
        nmlp = (hat2 * g2_ref[...]).astype(BF)
        s_nmlp[rows, :] = nmlp
        up = dot(nmlp, wup_ref[...])
        cdf = 0.5 * (1.0 + lax.erf(up * np.float32(np.sqrt(0.5))))
        slope = cdf + up * (jnp.exp(-0.5 * up * up) * np.float32(1 / np.sqrt(2 * np.pi)))
        hidden = (up * cdf).astype(BF)
        s_hidden[rows, :] = hidden
        after_mlp = (after + dot(hidden, wdown_ref[...])).astype(BF)

        spread = dot(perm_ref[...], after_mlp)
        parts = [spread[g * GPAD:(g + 1) * GPAD] for g in range(4)]
        average = sum(jnp.sum(p, axis=-1, keepdims=True) for p in parts) / (4 * C)
        parts = [p - average for p in parts]
        variance = sum(jnp.sum(p * p, axis=-1, keepdims=True) for p in parts) / (4 * C)
        scale = lax.rsqrt(variance + 1e-05)
        hats = [p * scale for p in parts]
        ct = ct_ref[t]
        merged = jnp.zeros((GPAD, 2 * C), F32)
        grads = []
        for g in range(4):
            gain = gm_ref[g:g + 1, :]
            weight = wm_ref[g * C:(g + 1) * C, :]
            nm = (hats[g] * gain).astype(BF)
            merged = merged + dot(nm, weight)
            s_merge[g * C:(g + 1) * C, :] += dot(nm, ct, TN)
            grads.append(dot(ct, weight, NT).astype(BF).astype(F32) * gain)
        merged_ref[t] = merged.astype(BF)
        first = sum(jnp.sum(g, axis=-1, keepdims=True) for g in grads) / (4 * C)
        second = sum(
            jnp.sum(g * hat, axis=-1, keepdims=True) for g, hat in zip(grads, hats)
        ) / (4 * C)
        back = jnp.concatenate(
            [scale * (g - first - hat * second) for g, hat in zip(grads, hats)], axis=0
        ).astype(BF)
        dy = dot(perm_ref[...], back, TN).astype(BF)

        s_dy[rows, :] = dy
        dhidden = dot(dy, wdown_ref[...], NT).astype(BF).astype(F32)
        du = (dhidden * slope).astype(BF)
        s_du[rows, :] = du
        dn = dot(du, wup_ref[...], NT).astype(BF).astype(F32) * g2_ref[...]
        da = (dy.astype(F32) + norm_grad(hat2, scale2, dn)).astype(BF)
        s_da[rows, :] = da

        dmixed[...] = dot(da, wproj_ref[...], NT).astype(BF)
        for h in range(HEADS):
            q = triple[0:WIN, h * HEAD:(h + 1) * HEAD]
            k = triple[:, C + h * HEAD:C + (h + 1) * HEAD]
            v = triple[:, 2 * C + h * HEAD:2 * C + (h + 1) * HEAD]
            dm = dmixed[:, h * HEAD:(h + 1) * HEAD]
            p = prob[h]
            dp = dot(dm, v, NT).astype(BF).astype(F32)
            ds = p * (dp - jnp.sum(dp * p, axis=-1, keepdims=True))
            where_rows = pl.ds(t * HEADS + h, WIN, stride=TH)
            dscore[0, where_rows, :] = ds[:, :LANES]
            dscore[1, where_rows, :] = ds[:, LANES:]
            dsb = (ds * root).astype(BF)
            dtriple[:, h * HEAD:(h + 1) * HEAD] = dot(dsb, k).astype(BF)
            dtriple[:, C + h * HEAD:C + (h + 1) * HEAD] = dot(dsb, q, TN)[:WIN].astype(BF)
            dtriple[:, 2 * C + h * HEAD:2 * C + (h + 1) * HEAD] = dot(
                p.astype(BF), dm, TN
            )[:WIN].astype(BF)
        dt = dtriple[...]
        s_dtriple[rows, :] = dt
        dn1 = dot(dt, wqkv_ref[...], NT).astype(BF).astype(F32) * g1_ref[...]
        fgrad_ref[rows, :] = (da.astype(F32) + norm_grad(hat1, scale1, dn1)).astype(BF)
        return carry

    lax.fori_loop(0, TYPES, one_type, 0)

    def pack(first_block, value):
        for b in range(value.shape[1] // LANES):
            start = (first_block + b) * C
            packed_ref[start:start + C, :] = value[:, b * LANES:(b + 1) * LANES].astype(BF)

    pack(0, jnp.concatenate(
        [dot(s_normed[...], s_dtriple[...], TN), dot(s_mixed[...], s_da[...], TN)], axis=1))
    pack(6, dot(s_nmlp[...], s_du[...], TN))
    down = dot(s_hidden[...], s_dy[...], TN)
    pack(12, jnp.concatenate([down[g * C:(g + 1) * C] for g in range(4)], axis=1))
    for g in range(4):
        pack(18 + 3 * g, s_merge[g * C:(g + 1) * C, :])

    s_table[...] = jnp.zeros_like(s_table)

    def some_rows(step, carry):
        hots, lefts = [], []
        for u in range(UNROLL):
            i = step * UNROLL + u
            lane = lane_ref[pl.ds(i, 1), :]
            digit = digit_ref[pl.ds(i, 1), :]
            hots.append((lax.broadcasted_iota(jnp.int32, (RADIX, KEYS), 0) == lane).astype(BF))
            rows = pl.ds(pl.multiple_of(i * TH, TH), TH)
            ds = jnp.concatenate([dscore[0, rows, :], dscore[1, rows, :]], axis=1)
            lefts.append(jnp.concatenate(
                [jnp.where(digit == d, ds, 0.0) for d in range(DIGITS)], axis=0
            ).astype(BF))
        s_table[...] += dot(
            jnp.concatenate(lefts, axis=1), jnp.concatenate(hots, axis=1), NT
        )
        return carry

    lax.fori_loop(0, WIN // UNROLL, some_rows, 0)
    for b in range(2):
        start = ROWS_W + b * DIGITS * TH
        packed_ref[start:start + DIGITS * TH, :] = s_table[:, b * LANES:(b + 1) * LANES].astype(BF)
    end = ROWS_W + ROWS_T
    if packed_ref.shape[0] > end:
        packed_ref[end:, :] = jnp.zeros((packed_ref.shape[0] - end, LANES), BF)


def reduce_kernel(
    n, share, factor, packed_ref,
    qkv_ref, proj_ref, up_ref, down_ref, merge_ref, table_ref,
    paired, pair_sum, arrived, gathered,
    send0, recv0, send1, recv1, send2, recv2, send3, recv3,
):
    chips = n // 2
    me = lax.axis_index("lon")
    chip, core = me // 2, lax.rem(me, 2)
    partner = 2 * chip + 1 - core

    def across(k):
        return 2 * lax.rem(chip + k, chips) + core

    def rows_of(half, index):
        return pl.ds(pl.multiple_of((half * chips + index) * share, 16), share)

    def sent(src, dst, send, recv, device):
        copy = pltpu.make_async_remote_copy(
            src_ref=src, dst_ref=dst, send_sem=send, recv_sem=recv,
            device_id={"lon": device}, device_id_type=pl.DeviceIdType.MESH,
        )
        copy.start()
        return copy

    barrier = pltpu.get_barrier_semaphore()
    for device in [partner] + [across(k) for k in range(1, chips)]:
        pl.semaphore_signal(
            barrier, inc=1, device_id={"lon": device}, device_id_type=pl.DeviceIdType.MESH
        )
    pl.semaphore_wait(barrier, chips)

    order = list(range(1, chips)) + [0]
    stage0 = {}
    for k in order:
        stage0[k] = sent(
            packed_ref.at[rows_of(1 - core, lax.rem(chip + k, chips)), :],
            paired.at[k], send0.at[k], recv0.at[k], partner,
        )
    stage1 = {}
    total = None
    for k in order:
        stage0[k].wait_recv()
        own = packed_ref[rows_of(core, lax.rem(chip + k, chips)), :].astype(F32)
        summed = own + paired[k].astype(F32)
        if k == 0:
            total = summed
        else:
            pair_sum[k] = summed.astype(BF)
            stage1[k] = sent(
                pair_sum.at[k], arrived.at[k], send1.at[k], recv1.at[k], across(k)
            )
    for k in range(1, chips):
        stage1[k].wait_recv()
        total = total + arrived[k].astype(F32)
    mine = rows_of(core, chip)
    gathered[mine, :] = total.astype(BF)
    stage2 = {}
    for k in range(1, chips):
        stage2[k] = sent(
            gathered.at[mine, :], gathered.at[mine, :], send2.at[k], recv2.at[k], across(k)
        )
    stage3 = [sent(
        gathered.at[mine, :], gathered.at[mine, :], send3.at[0], recv3.at[0], partner
    )]
    for k in range(1, chips):
        stage2[k].wait_recv()
        rows = rows_of(core, lax.rem(chip - k + chips, chips))
        stage3.append(sent(
            gathered.at[rows, :], gathered.at[rows, :], send3.at[k], recv3.at[k], partner
        ))
    for k in order:
        stage0[k].wait_send()
    for k in range(1, chips):
        stage1[k].wait_send()
        stage2[k].wait_send()
    for copy in stage3:
        copy.wait()

    def block(index):
        return gathered[index * C:(index + 1) * C, :].astype(F32) * factor

    def joined(start, count):
        return jnp.concatenate([block(start + b) for b in range(count)], axis=1)

    front = joined(0, 6)
    qkv_ref[...] = front[:, :3 * C]
    proj_ref[...] = front[:, 3 * C:]
    up_ref[...] = joined(6, 6)
    downs = joined(12, 6)
    for g in range(4):
        down_ref[g * C:(g + 1) * C, :] = downs[:, g * C:(g + 1) * C]
        merge_ref[g * C:(g + 1) * C, :] = joined(18 + 3 * g, 3)
    for b in range(2):
        start = ROWS_W + b * DIGITS * TH
        half = gathered[start:start + DIGITS * TH, :].astype(F32) * factor
        for d in range(DIGITS):
            at = d * RADIX + b * LANES
            table_ref[:, at:at + LANES] = half[d * TH:(d + 1) * TH]


def passed_along(value, axis, steps):
    count = lax.axis_size(axis)
    return lax.ppermute(value, axis, [(s, (s + steps) % count) for s in range(count)])


def group_order():
    order = np.zeros((4 * GPAD, WIN), np.float32)
    for pa in range(2):
        for pb in range(2):
            for z in range(WZ):
                for a in range(WLAT // 2):
                    for b in range(WLON // 2):
                        cell = (z * (WLAT // 2) + a) * (WLON // 2) + b
                        token = (z * WLAT + 2 * a + pa) * WLON + 2 * b + pb
                        order[(2 * pa + pb) * GPAD + cell, token] = 1.0
    return jnp.asarray(order, BF)


def local(
    fields, norm_gain, qkv_weight, proj_weight, bias_table, bias_index, region_ids,
    mlp_gain, up_weight, down_weight, merge_gain, merge_weight, cotangent,
):
    n = lax.axis_size("lon")
    windows = fields.shape[2] // WLON
    assert windows == 1
    bands = LAT // WLAT
    west_fields = passed_along(fields[:, :, :HALF], "lon", -1)
    west_ct = passed_along(cotangent[:, :, :HALF // 2], "lon", -1)

    table = jnp.pad(bias_table.reshape(TH, BPOS), ((0, 0), (0, DIGITS * RADIX - BPOS)))
    table = table.reshape(TH, DIGITS, RADIX).transpose(1, 0, 2).reshape(DIGITS * TH, RADIX)
    table = table.astype(BF)
    index = jnp.pad(bias_index, ((0, 0), (0, KEYS - WIN)), constant_values=-1)
    digit = index >> 8
    lane = jnp.where(index < 0, -1, index & (RADIX - 1))
    bias = pl.pallas_call(
        bias_kernel,
        out_shape=jax.ShapeDtypeStruct((2, WIN * TH, LANES), F32),
        in_specs=[VMEM] * 3,
        out_specs=VMEM,
        compiler_params=pltpu.CompilerParams(vmem_limit_bytes=24 << 20),
        cost_estimate=pl.CostEstimate(flops=7_000_000_000, bytes_accessed=4 << 20, transcendentals=0),
        name="bias_rows",
    )(table, digit, lane)

    labels = region_ids.reshape(WZ, bands, WLAT).transpose(1, 0, 2).reshape(TYPES, WZ * WLAT)
    labels = jnp.repeat(labels, WLON, axis=1)
    label_keys = jnp.pad(labels, ((0, 0), (0, KEYS - WIN)), constant_values=-1)

    shifted = jnp.concatenate([fields[:, :, HALF:], west_fields], axis=2)
    tokens = shifted.reshape(WZ, bands, WLAT, WLON, C).transpose(1, 0, 2, 3, 4).reshape(TYPES * WIN, C)
    ct = jnp.concatenate([cotangent[:, :, HALF // 2:], west_ct], axis=2)
    ct = ct.reshape(WZ, bands, WLAT // 2, WLON // 2, 2 * C).transpose(1, 0, 2, 3, 4)
    ct = jnp.pad(ct.reshape(TYPES, GROUP, 2 * C), ((0, 0), (0, GPAD - GROUP), (0, 0)))

    share = -(-(ROWS_W + ROWS_T) // (16 * n)) * 16
    total_rows = TYPES * WIN
    merged_win, fgrad_win, packed = pl.pallas_call(
        block_kernel,
        out_shape=(
            jax.ShapeDtypeStruct((TYPES, GPAD, 2 * C), BF),
            jax.ShapeDtypeStruct((total_rows, C), BF),
            jax.ShapeDtypeStruct((n * share, LANES), BF),
        ),
        in_specs=[VMEM] * 16,
        out_specs=(VMEM,) * 3,
        scratch_shapes=[
            pltpu.VMEM((KEYS, 3 * C), BF),
            pltpu.VMEM((HEADS, WIN, KEYS), F32),
            pltpu.VMEM((WIN, C), BF),
            pltpu.VMEM((WIN, C), BF),
            pltpu.VMEM((WIN, 3 * C), BF),
            pltpu.VMEM((2, WIN * TH, LANES), F32),
            pltpu.VMEM((total_rows, C), BF),
            pltpu.VMEM((total_rows, 3 * C), BF),
            pltpu.VMEM((total_rows, C), BF),
            pltpu.VMEM((total_rows, C), BF),
            pltpu.VMEM((total_rows, C), BF),
            pltpu.VMEM((total_rows, MLP), BF),
            pltpu.VMEM((total_rows, MLP), BF),
            pltpu.VMEM((total_rows, C), BF),
            pltpu.VMEM((4 * C, 2 * C), F32),
            pltpu.VMEM((DIGITS * TH, RADIX), F32),
        ],
        compiler_params=pltpu.CompilerParams(vmem_limit_bytes=48 << 20),
        cost_estimate=pl.CostEstimate(flops=20_000_000_000, bytes_accessed=8 << 20, transcendentals=2_000_000),
        name="block",
    )(
        tokens, ct, bias, labels[:, :, None], label_keys[:, None, :], digit, lane, group_order(),
        norm_gain[None], qkv_weight, proj_weight, mlp_gain[None], up_weight, down_weight,
        merge_gain.reshape(4, C), merge_weight,
    )

    merged_grid = merged_win[:, :GROUP].reshape(bands, WZ, WLAT // 2, WLON // 2, 2 * C)
    merged_grid = merged_grid.transpose(1, 0, 2, 3, 4).reshape(Z, LAT // 2, WLON // 2, 2 * C)
    fgrad_grid = fgrad_win.reshape(bands, WZ, WLAT, WLON, C)
    fgrad_grid = fgrad_grid.transpose(1, 0, 2, 3, 4).reshape(Z, LAT, WLON, C)
    east_merged = passed_along(merged_grid[:, :, HALF // 2:], "lon", 1)
    east_fgrad = passed_along(fgrad_grid[:, :, HALF:], "lon", 1)
    merged = jnp.concatenate([east_merged, merged_grid[:, :, :HALF // 2]], axis=2)
    field_grad = jnp.concatenate([east_fgrad, fgrad_grid[:, :, :HALF]], axis=2)

    factor = float(Z * LAT * fields.shape[2] * n) ** (-0.5)
    outs = pl.pallas_call(
        functools.partial(reduce_kernel, n, share, factor),
        out_shape=(
            jax.ShapeDtypeStruct((C, 3 * C), F32),
            jax.ShapeDtypeStruct((C, C), F32),
            jax.ShapeDtypeStruct((C, MLP), F32),
            jax.ShapeDtypeStruct((MLP, C), F32),
            jax.ShapeDtypeStruct((4 * C, 2 * C), F32),
            jax.ShapeDtypeStruct((TH, DIGITS * RADIX), F32),
        ),
        in_specs=[VMEM],
        out_specs=(VMEM,) * 6,
        scratch_shapes=[
            pltpu.VMEM((n // 2, share, LANES), BF),
            pltpu.VMEM((n // 2, share, LANES), BF),
            pltpu.VMEM((n // 2, share, LANES), BF),
            pltpu.VMEM((n * share, LANES), BF),
        ] + [pltpu.SemaphoreType.DMA((n // 2,))] * 8,
        compiler_params=pltpu.CompilerParams(
            collective_id=0, has_side_effects=True, vmem_limit_bytes=24 << 20
        ),
        cost_estimate=pl.CostEstimate(flops=10_000_000_000, bytes_accessed=16 << 20, transcendentals=0),
        name="weight_sums",
    )(packed)
    qkv_grad, proj_grad, up_grad, down_grad, merge_grad, table_grad = outs
    table_grad = table_grad[:, :BPOS].reshape(TYPES, HEADS, BPOS)
    return (
        merged, field_grad, qkv_grad, proj_grad, up_grad, down_grad, merge_grad, table_grad,
    )


def solution(mesh):
    grid = P("groups", None, "lon", None)
    rows = P("groups", None)
    return jax.shard_map(
        local,
        mesh=mesh,
        in_specs=(grid,) + (P(),) * 11 + (grid,),
        out_specs=(grid, grid) + (rows,) * 5 + (P("groups", None, None),),
        check_vma=False,
    )
```
